512 devices in a mesh: grp: 2 (over y), gy: 32 (over z), gx: 4 (over x), gz: 2 (over core).
Axes of the slice: x: 4, y: 2, z: 32, core: 2. Of those that a mesh axis runs over, the one named last changes fastest.
The devices are a block of a 4x8x32 slice.
Arguments:
- pair: bfloat16 [1024, 512, 128], P(('grp', 'gx', 'gz'), 'gy'), parts along dimension 0, may hold values from -6 to 6
- lengths: int32 [2], P('grp'), parts along dimension 0, may hold values from 256 to 512
- ln_gain: float32 [128], replicated, may hold values from 0.1 to 1.9
- ln_bias: float32 [128], replicated, may hold values from -3 to 3
- w_ab: bfloat16 [128, 512], replicated, may hold values from -0.5 to 0.5
- w_gate: bfloat16 [128, 128], replicated, may hold values from -0.5 to 0.5
- out_gain: float32 [128], replicated, may hold values from 0.1 to 1.9
- out_bias: float32 [128], replicated, may hold values from -3 to 3
- w_out: bfloat16 [128, 128], replicated, may hold values from -0.5 to 0.5
Outputs:
- update: bfloat16 [1024, 512, 128], P(('grp', 'gx', 'gz'), 'gy'), parts along dimension 0
The draws below stay inside these ranges and needn't reach their ends.
There are 2 independent parts, one for each index of `grp`. The reference program is written for one: setup_inputs(seed, part) draws one part's arguments, and reference() takes and returns one part's arrays. A program takes and returns all parts, laid end to end along the dimension named above; an argument that names none is the same for every part. Nothing has to cross between parts.
Inputs may be any that keep to these rules, and one draw needn't show every extreme that they name: Residues from lengths[0] on are padding.
All inputs are finite; a program needn't handle non-finite values.
Results may differ from the reference program's by a relative error of at most 0.0052.
Values may be sent and summed in bfloat16 or wider, within the bound.
No kernel may reach another device: no remote copies, remote signals or barrier semaphores. Data moves between devices by JAX's collectives and lax.ppermute only.
A program may use at most 128 MiB of HBM per device.

```python
import jax
import jax.numpy as jnp
from jax import lax

N = 512
C = 128
CH = 128


def shard_levels(key, dims, pieces, smallest, top_value):
    factor_of, own = 1.0, jax.random.fold_in(key, 6)
    for dim, parts in pieces:
        steps = jnp.exp(jax.random.uniform(jax.random.fold_in(own, dim), (parts,), jnp.float32, smallest / len(pieces), top_value / len(pieces)))
        factor_of = factor_of * jnp.repeat(steps, dims[dim] // parts).reshape([-1 if axis == dim else 1 for axis in range(len(dims))])
    return factor_of


def gaussian(rng, extent, scale, reach, pieces=(), kind=jnp.bfloat16):
    level = shard_levels(rng, extent, pieces, -0.22, 0.18) if pieces else 1.0
    array = jax.random.normal(rng, extent, jnp.float32) * scale * level
    return jnp.minimum(jnp.maximum(array, -reach), reach).astype(kind)


def setup_inputs(seed: int = 0, part: int = 0) -> dict:
    keys = jax.random.split(jax.random.key(seed), 10)
    part_keys = jax.random.split(jax.random.fold_in(keys[9], part), 10)
    pair = gaussian(part_keys[0], (N, N, C), 1.0, 6.0, ((0, 8), (1, 32)))
    lengths = jax.random.randint(part_keys[1], (1,), N // 2, N + 1).astype(jnp.int32)
    ln_gain = jnp.clip(1.0 + 0.18 * jax.random.normal(keys[2], (C,), jnp.float32), 0.1, 1.9)
    ln_bias = gaussian(keys[3], (C,), 0.5, 3.0, (), jnp.float32)
    w_ab = gaussian(keys[4], (C, 4 * CH), C ** -0.5, 0.5)
    w_gate = gaussian(keys[5], (C, C), C ** -0.5, 0.5)
    out_gain = jnp.clip(1.0 + 0.18 * jax.random.normal(keys[6], (CH,), jnp.float32), 0.1, 1.9)
    out_bias = gaussian(keys[7], (CH,), 0.5, 3.0, (), jnp.float32)
    w_out = gaussian(keys[8], (CH, C), CH ** -0.5, 0.5)
    return dict(pair=pair, lengths=lengths, ln_gain=ln_gain, ln_bias=ln_bias, w_ab=w_ab, w_gate=w_gate, out_gain=out_gain, out_bias=out_bias, w_out=w_out)


def layer_norm(values, gain, bias):
    values = values.astype(jnp.float32)
    mean = lax.optimization_barrier(jnp.mean(values, -1, keepdims=True))
    spread = lax.optimization_barrier(jnp.mean(jnp.square(values - mean), -1, keepdims=True))
    return (values - mean) * lax.rsqrt(spread + 1e-05) * gain.astype(jnp.float32) + bias.astype(jnp.float32)

def reference(pair, lengths, ln_gain, ln_bias, w_ab, w_gate, out_gain, out_bias, w_out):
    hidden = w_out.shape[0]
    width = pair.shape[2]
    normed = layer_norm(pair, ln_gain, ln_bias).astype(jnp.bfloat16)
    flat = normed.reshape(N * N, width)
    proj = jnp.dot(flat, w_ab, preferred_element_type=jnp.float32).reshape(N, N, 4 * hidden)
    live = (jnp.arange(N, dtype=jnp.int32) < lengths[0]).astype(jnp.float32)
    pair_mask = (live[:, None] * live[None, :])[..., None]
    left = (pair_mask * jax.nn.sigmoid(proj[..., :hidden]) * proj[..., hidden:2 * hidden]).astype(jnp.bfloat16)
    right = (pair_mask * jax.nn.sigmoid(proj[..., 2 * hidden:3 * hidden]) * proj[..., 3 * hidden:]).astype(jnp.bfloat16)
    triangle = jnp.einsum('ikc,jkc->ijc', left.astype(jnp.float32), right.astype(jnp.float32), precision=lax.Precision.HIGHEST)
    tri_norm = layer_norm(triangle, out_gain, out_bias).astype(jnp.bfloat16)
    gate = jax.nn.sigmoid(jnp.dot(flat, w_gate, preferred_element_type=jnp.float32))
    projected = jnp.dot(tri_norm.reshape(N * N, hidden), w_out, preferred_element_type=jnp.float32)
    return (gate * projected).astype(jnp.bfloat16).reshape(N, N, width)
```

```python
import functools

import jax
import jax.numpy as jnp
from jax import lax
from jax.experimental import pallas as pl
from jax.experimental.pallas import tpu as pltpu
from jax.sharding import PartitionSpec as P

NT = (((1,), (1,)), ((), ()))
TN = (((0,), (0,)), ((), ()))
EPS = 1e-05


def low_half(shape):
    return lax.broadcasted_iota(jnp.int32, shape, len(shape) - 1) < shape[-1] // 2


def swap_halves(value):
    return pltpu.roll(value, value.shape[-1] // 2, value.ndim - 1)


def pre_kernel(place, length, x_ref, gain, bias, w_ref, normed_ref, out_ref, rows_s, out_s):
    rows, cols, width = x_ref.shape
    hidden = w_ref.shape[1] // 4
    x = x_ref[...].reshape(rows * cols, width).astype(jnp.float32)
    mean = jnp.mean(x, -1, keepdims=True)
    x = x - mean
    spread = jnp.mean(x * x, -1, keepdims=True)
    normed = (x * lax.rsqrt(spread + EPS) * gain[...] + bias[...]).astype(jnp.bfloat16)
    normed_ref[...] = normed
    rows_s[...] = normed.astype(jnp.float32)
    w_t = w_ref[...].astype(jnp.float32).T.astype(jnp.bfloat16)
    low = low_half((1, 2 * rows))
    lane = lax.broadcasted_iota(jnp.int32, (1, 2 * rows), 1)
    row_live = place[0] + jnp.where(low, lane, lane - rows) < length[0]
    for pair in range(cols // 2):
        k = 2 * pair
        block = jnp.concatenate(
            [rows_s[pl.ds(k, rows, stride=cols), :], rows_s[pl.ds(k + 1, rows, stride=cols), :]], 0
        ).astype(jnp.bfloat16)
        proj = lax.dot_general(w_t, block, NT, preferred_element_type=jnp.float32)
        col_live = place[1] + k + jnp.where(low, 0, 1) < length[0]
        mask = jnp.where(row_live & col_live, 1.0, 0.0)
        left = mask * jax.nn.sigmoid(proj[:hidden]) * proj[hidden : 2 * hidden]
        right = mask * jax.nn.sigmoid(proj[2 * hidden : 3 * hidden]) * proj[3 * hidden :]
        out_s[pl.ds(k, hidden, stride=cols), :] = jnp.where(low, left, swap_halves(right))
        out_s[pl.ds(k + 1, hidden, stride=cols), :] = jnp.where(low, swap_halves(left), right)
    out_ref[...] = out_s[...].astype(jnp.bfloat16).reshape(out_ref.shape)


def mid_kernel(place, own_ref, peer_ref, out_ref):
    steps, blocks, depth, lanes = own_ref.shape
    half = lanes // 2

    def operand(ref, first):
        parts = [ref[:, x].reshape(steps * depth, lanes)[:, first : first + half] for x in range(blocks)]
        return jnp.concatenate(parts, 1)

    left = operand(own_ref, 0)
    low = low_half((1, 1, lanes))
    for which, ref in enumerate((own_ref, peer_ref)):
        core = place[2] if which == 0 else 1 - place[2]
        total = lax.dot_general(operand(ref, half), left, TN, preferred_element_type=jnp.float32)
        total = total.reshape(blocks * half // depth, depth, blocks * half)
        top, bottom = total[:, : depth // 2], total[:, depth // 2 :]
        for pair in range(blocks // 2):
            here = slice(pair * lanes, (pair + 1) * lanes)
            even = jnp.where(low, top[..., here], swap_halves(bottom[..., here]))
            odd = jnp.where(low, swap_halves(top[..., here]), bottom[..., here])
            tiles = jnp.concatenate([even, odd], 1).astype(jnp.bfloat16)
            out_ref[:, core, :, pair] = tiles.reshape(blocks, half // depth, depth, lanes)


def post_kernel(t_ref, gate, gain, bias, w_ref, out_ref, t_s, out_s):
    rows, cols, width = out_ref.shape
    hidden = w_ref.shape[0]
    depth = cols // 2
    t_s[...] = t_ref[...].astype(jnp.float32).reshape(t_s.shape)
    gain_t = jnp.broadcast_to(gain[...], (2 * rows, hidden)).T
    bias_t = jnp.broadcast_to(bias[...], (2 * rows, hidden)).T
    w = w_ref[...]
    for r in range(depth):
        t = t_s[pl.ds(r, hidden, stride=depth), :]
        t = t - jnp.mean(t, 0, keepdims=True)
        spread = jnp.mean(t * t, 0, keepdims=True)
        t = (t * lax.rsqrt(spread + EPS) * gain_t + bias_t).astype(jnp.bfloat16)
        o = lax.dot_general(t, w, TN, preferred_element_type=jnp.float32)
        out_s[pl.ds(r, rows, stride=cols), :] = o[:rows]
        out_s[pl.ds(depth + r, rows, stride=cols), :] = o[rows:]
    out_ref[...] = (gate[...] * out_s[...]).astype(jnp.bfloat16).reshape(out_ref.shape)


SMEM = pl.BlockSpec(memory_space=pltpu.SMEM)
VMEM = pl.BlockSpec(memory_space=pltpu.VMEM)


def body(pair, lengths, ln_gain, ln_bias, w_ab, w_gate, out_gain, out_bias, w_out):
    rows, cols, width = pair.shape
    hidden = w_out.shape[0]
    steps, blocks, cores = (lax.axis_size(a) for a in ("gy", "gx", "gz"))
    place = jnp.stack(
        [lax.axis_index(("gx", "gz")) * rows, lax.axis_index("gy") * cols, lax.axis_index("gz")]
    ).astype(jnp.int32)
    normed, operands = pl.pallas_call(
        pre_kernel,
        out_shape=(
            jax.ShapeDtypeStruct((rows * cols, width), jnp.bfloat16),
            jax.ShapeDtypeStruct((hidden, cols, 2 * rows), jnp.bfloat16),
        ),
        in_specs=[SMEM, SMEM, VMEM, VMEM, VMEM, VMEM],
        out_specs=(VMEM, VMEM),
        scratch_shapes=[
            pltpu.VMEM((rows * cols, width), jnp.float32),
            pltpu.VMEM((hidden * cols, 2 * rows), jnp.float32),
        ],
        name="pre",
    )(place, lengths, pair, ln_gain[None], ln_bias[None], w_ab)
    own = lax.all_to_all(operands, ("gy", "gx"), 0, 0, tiled=True)
    peer = lax.ppermute(own, "gz", [(g, cores - 1 - g) for g in range(cores)])
    gate = jax.nn.sigmoid(jnp.dot(normed, w_gate, preferred_element_type=jnp.float32))
    shape = (steps, blocks, cols, 2 * rows)
    tiles = pl.pallas_call(
        mid_kernel,
        out_shape=jax.ShapeDtypeStruct(
            (blocks, cores, rows // cols, blocks // 2, cols, 2 * rows), jnp.bfloat16
        ),
        in_specs=[SMEM, VMEM, VMEM],
        out_specs=VMEM,
        name="mid",
    )(place, own.reshape(shape), peer.reshape(shape))
    tiles = tiles.reshape(steps * blocks, cols // 2, 2 * rows)
    back = lax.all_to_all(tiles, ("gy", "gx"), 0, 0, tiled=True)
    return pl.pallas_call(
        post_kernel,
        out_shape=jax.ShapeDtypeStruct((rows, cols, width), jnp.bfloat16),
        in_specs=[VMEM] * 5,
        out_specs=VMEM,
        scratch_shapes=[
            pltpu.VMEM((hidden * cols // 2, 2 * rows), jnp.float32),
            pltpu.VMEM((rows * cols, width), jnp.float32),
        ],
        name="post",
    )(back.reshape(hidden // 2, cols, 2 * rows), gate, out_gain[None], out_bias[None], w_out)


def solution(mesh):
    in_specs = (P(("grp", "gx", "gz"), "gy", None), P("grp"), P(), P(), P(), P(), P(), P(), P())
    out_specs = P(("grp", "gx", "gz"), "gy", None)
    return jax.shard_map(body, mesh=mesh, in_specs=in_specs, out_specs=out_specs, check_vma=False)
```

```python
import functools

import jax
import jax.numpy as jnp
from jax import lax
from jax.experimental import pallas as pl
from jax.experimental.pallas import tpu as pltpu
from jax.sharding import PartitionSpec as P

NT = (((1,), (1,)), ((), ()))
TN = (((0,), (0,)), ((), ()))
EPS = 1e-05


def low_half(shape):
    return lax.broadcasted_iota(jnp.int32, shape, len(shape) - 1) < shape[-1] // 2


def swap_halves(value):
    return pltpu.roll(value, value.shape[-1] // 2, value.ndim - 1)


def pre_kernel(length, x_ref, gain, bias, w_ref, normed_ref, out_ref, rows_s, out_s):
    rows, cols, width = x_ref.shape
    hidden = w_ref.shape[1] // 4
    x = x_ref[...].reshape(rows * cols, width).astype(jnp.float32)
    mean = jnp.mean(x, -1, keepdims=True)
    x = x - mean
    spread = jnp.mean(x * x, -1, keepdims=True)
    normed = (x * lax.rsqrt(spread + EPS) * gain[...] + bias[...]).astype(jnp.bfloat16)
    normed_ref[...] = normed
    rows_s[...] = normed.astype(jnp.float32)
    w_t = w_ref[...].astype(jnp.float32).T.astype(jnp.bfloat16)
    low = low_half((1, 2 * rows))
    lane = lax.broadcasted_iota(jnp.int32, (1, 2 * rows), 1)
    row_start = (lax.axis_index("gx") * lax.axis_size("gz") + lax.axis_index("gz")) * rows
    col_start = lax.axis_index("gy") * cols
    row_live = row_start + jnp.where(low, lane, lane - rows) < length[0]
    for pair in range(cols // 2):
        k = 2 * pair
        block = jnp.concatenate(
            [rows_s[pl.ds(k, rows, stride=cols), :], rows_s[pl.ds(k + 1, rows, stride=cols), :]], 0
        ).astype(jnp.bfloat16)
        proj = lax.dot_general(w_t, block, NT, preferred_element_type=jnp.float32)
        col_live = col_start + k + jnp.where(low, 0, 1) < length[0]
        mask = jnp.where(row_live & col_live, 1.0, 0.0)
        left = mask * jax.nn.sigmoid(proj[:hidden]) * proj[hidden : 2 * hidden]
        right = mask * jax.nn.sigmoid(proj[2 * hidden : 3 * hidden]) * proj[3 * hidden :]
        out_s[pl.ds(k, hidden, stride=cols), :] = jnp.where(low, left, swap_halves(right))
        out_s[pl.ds(k + 1, hidden, stride=cols), :] = jnp.where(low, swap_halves(left), right)
    out_ref[...] = out_s[...].astype(jnp.bfloat16).reshape(out_ref.shape)


def operand(ref, first):
    steps, blocks, depth, lanes = ref.shape
    half = lanes // 2
    parts = [ref[:, x].reshape(steps * depth, lanes)[:, first : first + half] for x in range(blocks)]
    return jnp.concatenate(parts, 1)


def product(left, right, depth):
    lanes = 2 * left.shape[1] // 4
    half = lanes // 2
    low = low_half((1, 1, lanes))
    total = lax.dot_general(right, left, TN, preferred_element_type=jnp.float32)
    blocks = total.shape[1] // half
    total = total.reshape(total.shape[0] // depth, depth, blocks * half)
    top, bottom = total[:, : depth // 2], total[:, depth // 2 :]
    tiles = []
    for pair in range(blocks // 2):
        here = slice(pair * lanes, (pair + 1) * lanes)
        even = jnp.where(low, top[..., here], swap_halves(bottom[..., here]))
        odd = jnp.where(low, swap_halves(top[..., here]), bottom[..., here])
        tiles.append(jnp.concatenate([even, odd], 1).astype(jnp.bfloat16))
    return [t.reshape(blocks, t.shape[0] // blocks, depth, lanes) for t in tiles]


def own_kernel(own_ref, out_ref):
    half = own_ref.shape[3] // 2
    tiles = product(operand(own_ref, 0), operand(own_ref, half), own_ref.shape[2])
    for pair, tile in enumerate(tiles):
        out_ref[:, :, pair] = tile


def peer_kernel(own_ref, peer_ref, done_ref, out_ref):
    half = own_ref.shape[3] // 2
    core = lax.axis_index("gz")
    out_ref[:, core] = done_ref[...]
    tiles = product(operand(own_ref, 0), operand(peer_ref, half), own_ref.shape[2])
    for pair, tile in enumerate(tiles):
        out_ref[:, 1 - core, :, pair] = tile


def post_kernel(t_ref, normed, w_gate, gain, bias, w_ref, out_ref, t_s, out_s):
    rows, cols, width = out_ref.shape
    hidden = w_ref.shape[0]
    depth = cols // 2
    t_s[...] = t_ref[...].astype(jnp.float32).reshape(t_s.shape)
    gain_t = jnp.broadcast_to(gain[...], (2 * rows, hidden)).T
    bias_t = jnp.broadcast_to(bias[...], (2 * rows, hidden)).T
    w = w_ref[...]
    for r in range(depth):
        t = t_s[pl.ds(r, hidden, stride=depth), :]
        t = t - jnp.mean(t, 0, keepdims=True)
        spread = jnp.mean(t * t, 0, keepdims=True)
        t = (t * lax.rsqrt(spread + EPS) * gain_t + bias_t).astype(jnp.bfloat16)
        o = lax.dot_general(t, w, TN, preferred_element_type=jnp.float32)
        out_s[pl.ds(r, rows, stride=cols), :] = o[:rows]
        out_s[pl.ds(depth + r, rows, stride=cols), :] = o[rows:]
    gate = jax.nn.sigmoid(jnp.dot(normed[...], w_gate[...], preferred_element_type=jnp.float32))
    out_ref[...] = (gate * out_s[...]).astype(jnp.bfloat16).reshape(out_ref.shape)


SMEM = pl.BlockSpec(memory_space=pltpu.SMEM)
VMEM = pl.BlockSpec(memory_space=pltpu.VMEM)
PARAMS = pltpu.CompilerParams(vmem_limit_bytes=16 * 2**20)


def body(pair, lengths, ln_gain, ln_bias, w_ab, w_gate, out_gain, out_bias, w_out):
    rows, cols, width = pair.shape
    hidden = w_out.shape[0]
    steps, blocks, cores = (lax.axis_size(a) for a in ("gy", "gx", "gz"))
    normed, operands = pl.pallas_call(
        pre_kernel,
        out_shape=(
            jax.ShapeDtypeStruct((rows * cols, width), jnp.bfloat16),
            jax.ShapeDtypeStruct((hidden, cols, 2 * rows), jnp.bfloat16),
        ),
        in_specs=[SMEM, VMEM, VMEM, VMEM, VMEM],
        compiler_params=PARAMS,
        out_specs=(VMEM, VMEM),
        scratch_shapes=[
            pltpu.VMEM((rows * cols, width), jnp.float32),
            pltpu.VMEM((hidden * cols, 2 * rows), jnp.float32),
        ],
        name="pre",
    )(lengths, pair, ln_gain[None], ln_bias[None], w_ab)
    own = lax.all_to_all(operands, ("gy", "gx"), 0, 0, tiled=True)
    peer = lax.ppermute(own, "gz", [(g, cores - 1 - g) for g in range(cores)])
    shape = (steps, blocks, cols, 2 * rows)
    own, peer = own.reshape(shape), peer.reshape(shape)
    group = (blocks, rows // cols, blocks // 2, cols, 2 * rows)
    tiles = pl.pallas_call(
        own_kernel,
        out_shape=jax.ShapeDtypeStruct(group, jnp.bfloat16),
        in_specs=[VMEM],
        out_specs=VMEM,
        compiler_params=PARAMS,
        cost_estimate=pl.CostEstimate(flops=2**30, bytes_accessed=2**20, transcendentals=0),
        name="own",
    )(own)
    tiles = pl.pallas_call(
        peer_kernel,
        out_shape=jax.ShapeDtypeStruct((blocks, cores, *group[1:]), jnp.bfloat16),
        in_specs=[VMEM] * 3,
        out_specs=VMEM,
        compiler_params=PARAMS,
        name="peer",
    )(own, peer, tiles)
    tiles = tiles.reshape(steps * blocks, cols // 2, 2 * rows)
    back = lax.all_to_all(tiles, ("gy", "gx"), 0, 0, tiled=True)
    return pl.pallas_call(
        post_kernel,
        out_shape=jax.ShapeDtypeStruct((rows, cols, width), jnp.bfloat16),
        in_specs=[VMEM] * 6,
        out_specs=VMEM,
        compiler_params=PARAMS,
        scratch_shapes=[
            pltpu.VMEM((hidden * cols // 2, 2 * rows), jnp.float32),
            pltpu.VMEM((rows * cols, width), jnp.float32),
        ],
        name="post",
    )(back.reshape(hidden // 2, cols, 2 * rows), normed, w_gate, out_gain[None], out_bias[None], w_out)


def solution(mesh):
    in_specs = (P(("grp", "gx", "gz"), "gy", None), P("grp"), P(), P(), P(), P(), P(), P(), P())
    out_specs = P(("grp", "gx", "gz"), "gy", None)
    return jax.shard_map(body, mesh=mesh, in_specs=in_specs, out_specs=out_specs, check_vma=False)
```

```python
import functools

import jax
import jax.numpy as jnp
from jax import lax
from jax.experimental import pallas as pl
from jax.experimental.pallas import tpu as pltpu
from jax.sharding import PartitionSpec as P

NT = (((1,), (1,)), ((), ()))
TN = (((0,), (0,)), ((), ()))
EPS = 1e-05


def low_half(shape):
    return lax.broadcasted_iota(jnp.int32, shape, len(shape) - 1) < shape[-1] // 2


def swap_halves(value):
    return pltpu.roll(value, value.shape[-1] // 2, value.ndim - 1)


def center_kernel(x_ref, out_ref):
    x = x_ref[...].reshape(out_ref.shape).astype(jnp.float32)
    x = x - jnp.mean(x, -1, keepdims=True)
    spread = jnp.mean(x * x, -1, keepdims=True)
    out_ref[...] = x * lax.rsqrt(spread + EPS)


def pre_kernel(length, x_ref, gain, bias, w_ref, normed_ref, out_ref, rows_s, out_s):
    hidden, cols, rows = out_ref.shape
    rows = rows // 2
    normed = (x_ref[...] * gain[...] + bias[...]).astype(jnp.bfloat16)
    normed_ref[...] = normed
    rows_s[...] = normed.astype(jnp.float32)
    w_t = w_ref[...].astype(jnp.float32).T.astype(jnp.bfloat16)
    low = low_half((1, 2 * rows))
    lane = lax.broadcasted_iota(jnp.int32, (1, 2 * rows), 1)
    row_start = (lax.axis_index("gx") * lax.axis_size("gz") + lax.axis_index("gz")) * rows
    col_start = lax.axis_index("gy") * cols
    row_live = row_start + jnp.where(low, lane, lane - rows) < length[0]
    for pair in range(cols // 2):
        k = 2 * pair
        block = jnp.concatenate(
            [rows_s[pl.ds(k, rows, stride=cols), :], rows_s[pl.ds(k + 1, rows, stride=cols), :]], 0
        ).astype(jnp.bfloat16)
        proj = lax.dot_general(w_t, block, NT, preferred_element_type=jnp.float32)
        col_live = col_start + k + jnp.where(low, 0, 1) < length[0]
        mask = jnp.where(row_live & col_live, 1.0, 0.0)
        left = mask * jax.nn.sigmoid(proj[:hidden]) * proj[hidden : 2 * hidden]
        right = mask * jax.nn.sigmoid(proj[2 * hidden : 3 * hidden]) * proj[3 * hidden :]
        out_s[pl.ds(k, hidden, stride=cols), :] = jnp.where(low, left, swap_halves(right))
        out_s[pl.ds(k + 1, hidden, stride=cols), :] = jnp.where(low, swap_halves(left), right)
    out_ref[...] = out_s[...].astype(jnp.bfloat16).reshape(out_ref.shape)


def operand(ref, first):
    steps, blocks, depth, lanes = ref.shape
    half = lanes // 2
    parts = [ref[:, x].reshape(steps * depth, lanes)[:, first : first + half] for x in range(blocks)]
    return jnp.concatenate(parts, 1)


def product(left, right, depth):
    lanes = 2 * left.shape[1] // 4
    half = lanes // 2
    low = low_half((1, 1, lanes))
    total = lax.dot_general(right, left, TN, preferred_element_type=jnp.float32)
    blocks = total.shape[1] // half
    total = total.reshape(total.shape[0] // depth, depth, blocks * half)
    top, bottom = total[:, : depth // 2], total[:, depth // 2 :]
    tiles = []
    for pair in range(blocks // 2):
        here = slice(pair * lanes, (pair + 1) * lanes)
        even = jnp.where(low, top[..., here], swap_halves(bottom[..., here]))
        odd = jnp.where(low, swap_halves(top[..., here]), bottom[..., here])
        tiles.append(jnp.concatenate([even, odd], 1).astype(jnp.bfloat16))
    return [t.reshape(blocks, t.shape[0] // blocks, depth, lanes) for t in tiles]


def own_kernel(own_ref, normed, w_gate, gain, bias, out_ref, gate_ref, gain_t, bias_t):
    half = own_ref.shape[3] // 2
    tiles = product(operand(own_ref, 0), operand(own_ref, half), own_ref.shape[2])
    for pair, tile in enumerate(tiles):
        out_ref[:, :, pair] = tile
    gate_ref[...] = jax.nn.sigmoid(jnp.dot(normed[...], w_gate[...], preferred_element_type=jnp.float32))
    gain_t[...] = jnp.broadcast_to(gain[...], gain_t.shape[::-1]).T
    bias_t[...] = jnp.broadcast_to(bias[...], bias_t.shape[::-1]).T


def peer_kernel(own_ref, peer_ref, done_ref, out_ref):
    half = own_ref.shape[3] // 2
    core = lax.axis_index("gz")
    out_ref[:, core] = done_ref[...]
    tiles = product(operand(own_ref, 0), operand(peer_ref, half), own_ref.shape[2])
    for pair, tile in enumerate(tiles):
        out_ref[:, 1 - core, :, pair] = tile


def post_kernel(t_ref, gate, gain_t, bias_t, w_ref, out_hbm, t_s, out_s, out_v, sems):
    rows, cols, width = out_v.shape
    hidden = w_ref.shape[0]
    depth = cols // 2
    t_s[...] = t_ref[...].astype(jnp.float32).reshape(t_s.shape)
    w = w_ref[...]
    for r in range(depth):
        t = t_s[pl.ds(r, hidden, stride=depth), :]
        t = t - jnp.mean(t, 0, keepdims=True)
        spread = jnp.mean(t * t, 0, keepdims=True)
        t = (t * lax.rsqrt(spread + EPS) * gain_t[...] + bias_t[...]).astype(jnp.bfloat16)
        o = lax.dot_general(t, w, TN, preferred_element_type=jnp.float32)
        out_s[pl.ds(r, rows, stride=cols), :] = o[:rows]
        out_s[pl.ds(depth + r, rows, stride=cols), :] = o[rows:]
    parts = sems.shape[0]
    step = rows // parts
    copies = []
    for p in range(parts):
        here = pl.ds(p * step * cols, step * cols)
        out_v[pl.ds(p * step, step)] = (
            (gate[here] * out_s[here]).astype(jnp.bfloat16).reshape(step, cols, width)
        )
        copies.append(
            pltpu.make_async_copy(
                out_v.at[pl.ds(p * step, step)], out_hbm.at[pl.ds(p * step, step)], sems.at[p]
            )
        )
        copies[-1].start()
    for copy in copies:
        copy.wait()


SMEM = pl.BlockSpec(memory_space=pltpu.SMEM)
VMEM = pl.BlockSpec(memory_space=pltpu.VMEM)
HBM = pl.BlockSpec(memory_space=pltpu.HBM)
COST = pl.CostEstimate(flops=2**30, bytes_accessed=2**20, transcendentals=0)
PARAMS = pltpu.CompilerParams(vmem_limit_bytes=16 * 2**20)


def body(pair, lengths, ln_gain, ln_bias, w_ab, w_gate, out_gain, out_bias, w_out):
    rows, cols, width = pair.shape
    hidden = w_out.shape[0]
    steps, blocks, cores = (lax.axis_size(a) for a in ("gy", "gx", "gz"))
    parts = 4
    flat, square = (rows * cols, width), (hidden, 2 * rows)
    centered = pl.pallas_call(
        center_kernel,
        out_shape=jax.ShapeDtypeStruct(flat, jnp.float32),
        in_specs=[VMEM],
        out_specs=VMEM,
        compiler_params=PARAMS,
        cost_estimate=COST,
        name="center",
    )(pair)
    normed, operands = pl.pallas_call(
        pre_kernel,
        out_shape=(
            jax.ShapeDtypeStruct(flat, jnp.bfloat16),
            jax.ShapeDtypeStruct((hidden, cols, 2 * rows), jnp.bfloat16),
        ),
        in_specs=[SMEM] + [VMEM] * 4,
        out_specs=(VMEM, VMEM),
        scratch_shapes=[
            pltpu.VMEM(flat, jnp.float32),
            pltpu.VMEM((hidden * cols, 2 * rows), jnp.float32),
        ],
        compiler_params=PARAMS,
        cost_estimate=COST,
        name="pre",
    )(lengths, centered, ln_gain[None], ln_bias[None], w_ab)
    own = lax.all_to_all(operands, ("gy", "gx"), 0, 0, tiled=True)
    peer = lax.ppermute(own, "gz", [(g, cores - 1 - g) for g in range(cores)])
    shape = (steps, blocks, cols, 2 * rows)
    own, peer = own.reshape(shape), peer.reshape(shape)
    group = (blocks, rows // cols, blocks // 2, cols, 2 * rows)
    tiles, gate, gain_t, bias_t = pl.pallas_call(
        own_kernel,
        out_shape=(
            jax.ShapeDtypeStruct(group, jnp.bfloat16),
            jax.ShapeDtypeStruct(flat, jnp.float32),
            jax.ShapeDtypeStruct(square, jnp.float32),
            jax.ShapeDtypeStruct(square, jnp.float32),
        ),
        in_specs=[VMEM] * 5,
        out_specs=(VMEM,) * 4,
        compiler_params=PARAMS,
        cost_estimate=COST,
        name="own",
    )(own, normed, w_gate, out_gain[None], out_bias[None])
    tiles = pl.pallas_call(
        peer_kernel,
        out_shape=jax.ShapeDtypeStruct((blocks, cores, *group[1:]), jnp.bfloat16),
        in_specs=[VMEM] * 3,
        out_specs=VMEM,
        compiler_params=PARAMS,
        cost_estimate=COST,
        name="peer",
    )(own, peer, tiles)
    tiles = tiles.reshape(steps * blocks, cols // 2, 2 * rows)
    back = lax.all_to_all(tiles, ("gy", "gx"), 0, 0, tiled=True)
    return pl.pallas_call(
        post_kernel,
        out_shape=jax.ShapeDtypeStruct((rows, cols, width), jnp.bfloat16),
        in_specs=[VMEM] * 5,
        out_specs=HBM,
        scratch_shapes=[
            pltpu.VMEM((hidden * cols // 2, 2 * rows), jnp.float32),
            pltpu.VMEM(flat, jnp.float32),
            pltpu.VMEM((rows, cols, width), jnp.bfloat16),
            pltpu.SemaphoreType.DMA((parts,)),
        ],
        compiler_params=PARAMS,
        name="post",
    )(back.reshape(hidden // 2, cols, 2 * rows), gate, gain_t, bias_t, w_out)


def solution(mesh):
    in_specs = (P(("grp", "gx", "gz"), "gy", None), P("grp"), P(), P(), P(), P(), P(), P(), P())
    out_specs = P(("grp", "gx", "gz"), "gy", None)
    return jax.shard_map(body, mesh=mesh, in_specs=in_specs, out_specs=out_specs, check_vma=False)
```

```python
import functools

import jax
import jax.numpy as jnp
from jax import lax
from jax.experimental import pallas as pl
from jax.experimental.pallas import tpu as pltpu
from jax.sharding import PartitionSpec as P

NT = (((1,), (1,)), ((), ()))
TN = (((0,), (0,)), ((), ()))
EPS = 1e-05


def low_half(shape):
    return lax.broadcasted_iota(jnp.int32, shape, len(shape) - 1) < shape[-1] // 2


def swap_halves(value):
    return pltpu.roll(value, value.shape[-1] // 2, value.ndim - 1)


def center_kernel(x_ref, out_ref, rows_s):
    cols, rows, width = out_ref.shape
    x = x_ref[...].reshape(rows * cols, width).astype(jnp.float32)
    x = x - jnp.mean(x, -1, keepdims=True)
    spread = jnp.mean(x * x, -1, keepdims=True)
    rows_s[...] = x * lax.rsqrt(spread + EPS)
    for k in range(cols):
        out_ref[k] = rows_s[pl.ds(k, rows, stride=cols), :]


def pre_kernel(length, x_ref, gain, bias, w_ref, normed_ref, out_ref, out_s):
    cols, rows, width = x_ref.shape
    hidden = out_ref.shape[0]
    w_t = w_ref[...].astype(jnp.float32).T.astype(jnp.bfloat16)
    low = low_half((1, 2 * rows))
    lane = lax.broadcasted_iota(jnp.int32, (1, 2 * rows), 1)
    row_start = (lax.axis_index("gx") * lax.axis_size("gz") + lax.axis_index("gz")) * rows
    col_start = lax.axis_index("gy") * cols
    row_live = row_start + jnp.where(low, lane, lane - rows) < length[...]
    for k in range(0, cols, 2):
        block = x_ref[pl.ds(k, 2)].reshape(2 * rows, width)
        block = (block * gain[...] + bias[...]).astype(jnp.bfloat16)
        normed_ref[pl.ds(k * rows, 2 * rows)] = block
        proj = lax.dot_general(w_t, block, NT, preferred_element_type=jnp.float32)
        col_live = col_start + k + jnp.where(low, 0, 1) < length[...]
        mask = jnp.where(row_live & col_live, 1.0, 0.0)
        left = mask * jax.nn.sigmoid(proj[:hidden]) * proj[hidden : 2 * hidden]
        right = mask * jax.nn.sigmoid(proj[2 * hidden : 3 * hidden]) * proj[3 * hidden :]
        out_s[pl.ds(k, hidden, stride=cols), :] = jnp.where(low, left, swap_halves(right))
        out_s[pl.ds(k + 1, hidden, stride=cols), :] = jnp.where(low, swap_halves(left), right)
    out_ref[...] = out_s[...].astype(jnp.bfloat16).reshape(out_ref.shape)


def operand(ref, first):
    steps, blocks, depth, lanes = ref.shape
    half = lanes // 2
    parts = [ref[:, x].reshape(steps * depth, lanes)[:, first : first + half] for x in range(blocks)]
    return jnp.concatenate(parts, 1)


def product(left, right, depth):
    lanes = 2 * left.shape[1] // 4
    half = lanes // 2
    low = low_half((1, 1, lanes))
    total = lax.dot_general(right, left, TN, preferred_element_type=jnp.float32)
    blocks = total.shape[1] // half
    total = total.reshape(total.shape[0] // depth, depth, blocks * half)
    top, bottom = total[:, : depth // 2], total[:, depth // 2 :]
    tiles = []
    for pair in range(blocks // 2):
        here = slice(pair * lanes, (pair + 1) * lanes)
        even = jnp.where(low, top[..., here], swap_halves(bottom[..., here]))
        odd = jnp.where(low, swap_halves(top[..., here]), bottom[..., here])
        tiles.append(jnp.concatenate([even, odd], 1).astype(jnp.bfloat16))
    return [t.reshape(blocks, t.shape[0] // blocks, depth, lanes) for t in tiles]


def own_kernel(own_ref, normed, w_gate, gain, bias, out_ref, gate_ref, gain_t, bias_t):
    half = own_ref.shape[3] // 2
    tiles = product(operand(own_ref, 0), operand(own_ref, half), own_ref.shape[2])
    for pair, tile in enumerate(tiles):
        out_ref[:, :, pair] = tile
    gate_ref[...] = jax.nn.sigmoid(jnp.dot(normed[...], w_gate[...], preferred_element_type=jnp.float32))
    gain_t[...] = jnp.broadcast_to(gain[...], gain_t.shape[::-1]).T
    bias_t[...] = jnp.broadcast_to(bias[...], bias_t.shape[::-1]).T


def peer_kernel(own_ref, peer_ref, done_ref, out_ref):
    half = own_ref.shape[3] // 2
    core = lax.axis_index("gz")
    out_ref[:, core] = done_ref[...]
    tiles = product(operand(own_ref, 0), operand(peer_ref, half), own_ref.shape[2])
    for pair, tile in enumerate(tiles):
        out_ref[:, 1 - core, :, pair] = tile


def post_kernel(t_ref, gate, gain_t, bias_t, w_ref, out_hbm, t_s, out_s, out_v, sems):
    rows, cols, width = out_v.shape
    hidden = w_ref.shape[0]
    depth = cols // 2
    t_s[...] = t_ref[...].astype(jnp.float32).reshape(t_s.shape)
    w = w_ref[...]
    for r in range(depth):
        t = t_s[pl.ds(r, hidden, stride=depth), :]
        t = t - jnp.mean(t, 0, keepdims=True)
        spread = jnp.mean(t * t, 0, keepdims=True)
        t = (t * lax.rsqrt(spread + EPS) * gain_t[...] + bias_t[...]).astype(jnp.bfloat16)
        o = lax.dot_general(t, w, TN, preferred_element_type=jnp.float32)
        for half, col in enumerate((r, depth + r)):
            here = slice(half * rows, (half + 1) * rows)
            out_s[pl.ds(col, rows, stride=cols), :] = gate[pl.ds(col * rows, rows)] * o[here]
    parts = sems.shape[0]
    step = rows // parts
    copies = []
    for p in range(parts):
        here = pl.ds(p * step * cols, step * cols)
        out_v[pl.ds(p * step, step)] = (
            out_s[here].astype(jnp.bfloat16).reshape(step, cols, width)
        )
        copies.append(
            pltpu.make_async_copy(
                out_v.at[pl.ds(p * step, step)], out_hbm.at[pl.ds(p * step, step)], sems.at[p]
            )
        )
        copies[-1].start()
    for copy in copies:
        copy.wait()


VMEM = pl.BlockSpec(memory_space=pltpu.VMEM)
HBM = pl.BlockSpec(memory_space=pltpu.HBM)
COST = pl.CostEstimate(flops=2**30, bytes_accessed=2**20, transcendentals=0)
PARAMS = pltpu.CompilerParams(vmem_limit_bytes=16 * 2**20)


def body(pair, lengths, ln_gain, ln_bias, w_ab, w_gate, out_gain, out_bias, w_out):
    rows, cols, width = pair.shape
    hidden = w_out.shape[0]
    steps, blocks, cores = (lax.axis_size(a) for a in ("gy", "gx", "gz"))
    parts = 4
    flat, square = (rows * cols, width), (hidden, 2 * rows)
    centered = pl.pallas_call(
        center_kernel,
        out_shape=jax.ShapeDtypeStruct((cols, rows, width), jnp.float32),
        in_specs=[VMEM],
        out_specs=VMEM,
        scratch_shapes=[pltpu.VMEM(flat, jnp.float32)],
        compiler_params=PARAMS,
        cost_estimate=COST,
        name="center",
    )(pair)
    normed, operands = pl.pallas_call(
        pre_kernel,
        out_shape=(
            jax.ShapeDtypeStruct(flat, jnp.bfloat16),
            jax.ShapeDtypeStruct((hidden, cols, 2 * rows), jnp.bfloat16),
        ),
        in_specs=[VMEM] * 5,
        out_specs=(VMEM, VMEM),
        scratch_shapes=[pltpu.VMEM((hidden * cols, 2 * rows), jnp.float32)],
        compiler_params=PARAMS,
        cost_estimate=COST,
        name="pre",
    )(lengths[None], centered, ln_gain[None], ln_bias[None], w_ab)
    own = lax.all_to_all(operands, ("gy", "gx"), 0, 0, tiled=True)
    peer = lax.ppermute(own, "gz", [(g, cores - 1 - g) for g in range(cores)])
    shape = (steps, blocks, cols, 2 * rows)
    own, peer = own.reshape(shape), peer.reshape(shape)
    group = (blocks, rows // cols, blocks // 2, cols, 2 * rows)
    tiles, gate, gain_t, bias_t = pl.pallas_call(
        own_kernel,
        out_shape=(
            jax.ShapeDtypeStruct(group, jnp.bfloat16),
            jax.ShapeDtypeStruct(flat, jnp.float32),
            jax.ShapeDtypeStruct(square, jnp.float32),
            jax.ShapeDtypeStruct(square, jnp.float32),
        ),
        in_specs=[VMEM] * 5,
        out_specs=(VMEM,) * 4,
        compiler_params=PARAMS,
        cost_estimate=COST,
        name="own",
    )(own, normed, w_gate, out_gain[None], out_bias[None])
    tiles = pl.pallas_call(
        peer_kernel,
        out_shape=jax.ShapeDtypeStruct((blocks, cores, *group[1:]), jnp.bfloat16),
        in_specs=[VMEM] * 3,
        out_specs=VMEM,
        compiler_params=PARAMS,
        cost_estimate=COST,
        name="peer",
    )(own, peer, tiles)
    tiles = tiles.reshape(steps * blocks, cols // 2, 2 * rows)
    back = lax.all_to_all(tiles, ("gy", "gx"), 0, 0, tiled=True)
    return pl.pallas_call(
        post_kernel,
        out_shape=jax.ShapeDtypeStruct((rows, cols, width), jnp.bfloat16),
        in_specs=[VMEM] * 5,
        out_specs=HBM,
        scratch_shapes=[
            pltpu.VMEM((hidden * cols // 2, 2 * rows), jnp.float32),
            pltpu.VMEM(flat, jnp.float32),
            pltpu.VMEM((rows, cols, width), jnp.bfloat16),
            pltpu.SemaphoreType.DMA((parts,)),
        ],
        compiler_params=PARAMS,
        name="post",
    )(back.reshape(hidden // 2, cols, 2 * rows), gate, gain_t, bias_t, w_out)


def solution(mesh):
    in_specs = (P(("grp", "gx", "gz"), "gy", None), P("grp"), P(), P(), P(), P(), P(), P(), P())
    out_specs = P(("grp", "gx", "gz"), "gy", None)
    return jax.shard_map(body, mesh=mesh, in_specs=in_specs, out_specs=out_specs, check_vma=False)
```

```python
import functools

import jax
import jax.numpy as jnp
from jax import lax
from jax.experimental import pallas as pl
from jax.experimental.pallas import tpu as pltpu
from jax.sharding import PartitionSpec as P

NT = (((1,), (1,)), ((), ()))
TN = (((0,), (0,)), ((), ()))
EPS = 1e-05


def low_half(shape):
    return lax.broadcasted_iota(jnp.int32, shape, len(shape) - 1) < shape[-1] // 2


def swap_halves(value):
    return pltpu.roll(value, value.shape[-1] // 2, value.ndim - 1)


def center_kernel(x_ref, out_ref, rows_s):
    cols, rows, width = out_ref.shape
    x = x_ref[...].reshape(rows * cols, width).astype(jnp.float32)
    x = x - jnp.mean(x, -1, keepdims=True)
    spread = jnp.mean(x * x, -1, keepdims=True)
    rows_s[...] = x * lax.rsqrt(spread + EPS)
    for k in range(cols):
        out_ref[k] = rows_s[pl.ds(k, rows, stride=cols), :]


def pre_kernel(x_ref, gain, bias, w_ref, normed_ref, out_ref, out_s):
    cols, rows, width = x_ref.shape
    hidden = out_ref.shape[0]
    w_t = w_ref[...].astype(jnp.float32).T.astype(jnp.bfloat16)
    low = low_half((1, 2 * rows))
    for k in range(0, cols, 2):
        block = x_ref[pl.ds(k, 2)].reshape(2 * rows, width)
        block = (block * gain[...] + bias[...]).astype(jnp.bfloat16)
        normed_ref[pl.ds(k * rows, 2 * rows)] = block
        proj = lax.dot_general(w_t, block, NT, preferred_element_type=jnp.float32)
        left = jax.nn.sigmoid(proj[:hidden]) * proj[hidden : 2 * hidden]
        right = jax.nn.sigmoid(proj[2 * hidden : 3 * hidden]) * proj[3 * hidden :]
        out_s[pl.ds(k, hidden, stride=cols), :] = jnp.where(low, left, swap_halves(right))
        out_s[pl.ds(k + 1, hidden, stride=cols), :] = jnp.where(low, swap_halves(left), right)
    out_ref[...] = out_s[...].astype(jnp.bfloat16).reshape(out_ref.shape)


def operand(ref, first, length, core, mask_k):
    steps, blocks, depth, lanes = ref.shape
    half = lanes // 2
    parts = [ref[:, x].reshape(steps * depth, lanes)[:, first : first + half] for x in range(blocks)]
    value = jnp.concatenate(parts, 1)
    lane = lax.broadcasted_iota(jnp.int32, (1, blocks * half), 1)
    live = lane // half * (lax.axis_size("gz") * half) + core * half + lane % half < length
    if mask_k:
        live = live & (lax.broadcasted_iota(jnp.int32, (steps * depth, 1), 0) < length)
    return value * jnp.where(live, 1.0, 0.0).astype(jnp.bfloat16)


def product(left, right, depth):
    lanes = 2 * left.shape[1] // 4
    half = lanes // 2
    low = low_half((1, 1, lanes))
    total = lax.dot_general(right, left, TN, preferred_element_type=jnp.float32)
    blocks = total.shape[1] // half
    total = total.reshape(total.shape[0] // depth, depth, blocks * half)
    top, bottom = total[:, : depth // 2], total[:, depth // 2 :]
    tiles = []
    for pair in range(blocks // 2):
        here = slice(pair * lanes, (pair + 1) * lanes)
        even = jnp.where(low, top[..., here], swap_halves(bottom[..., here]))
        odd = jnp.where(low, swap_halves(top[..., here]), bottom[..., here])
        tiles.append(jnp.concatenate([even, odd], 1).astype(jnp.bfloat16))
    return [t.reshape(blocks, t.shape[0] // blocks, depth, lanes) for t in tiles]


def own_kernel(length, own_ref, normed, w_gate, gain, bias, out_ref, left_ref, gate_ref, gain_t, bias_t):
    half = own_ref.shape[3] // 2
    core = lax.axis_index("gz")
    left = operand(own_ref, 0, length[0], core, True)
    left_ref[...] = left
    tiles = product(left, operand(own_ref, half, length[0], core, False), own_ref.shape[2])
    for pair, tile in enumerate(tiles):
        out_ref[:, :, pair] = tile
    gate_ref[...] = jax.nn.sigmoid(jnp.dot(normed[...], w_gate[...], preferred_element_type=jnp.float32))
    gain_t[...] = jnp.broadcast_to(gain[...], gain_t.shape[::-1]).T
    bias_t[...] = jnp.broadcast_to(bias[...], bias_t.shape[::-1]).T


def peer_kernel(length, left_ref, peer_ref, done_ref, out_ref):
    half = peer_ref.shape[3] // 2
    core = lax.axis_index("gz")
    out_ref[:, core] = done_ref[...]
    right = operand(peer_ref, half, length[0], 1 - core, False)
    for pair, tile in enumerate(product(left_ref[...], right, peer_ref.shape[2])):
        out_ref[:, 1 - core, :, pair] = tile


def post_kernel(t_ref, gate, gain_t, bias_t, w_ref, out_hbm, t_s, out_s, out_v, sems):
    rows, cols, width = out_v.shape
    hidden = w_ref.shape[0]
    depth = cols // 2
    t_s[...] = t_ref[...].astype(jnp.float32).reshape(t_s.shape)
    w = w_ref[...]
    for r in range(depth):
        t = t_s[pl.ds(r, hidden, stride=depth), :]
        t = t - jnp.mean(t, 0, keepdims=True)
        spread = jnp.mean(t * t, 0, keepdims=True)
        t = (t * lax.rsqrt(spread + EPS) * gain_t[...] + bias_t[...]).astype(jnp.bfloat16)
        o = lax.dot_general(t, w, TN, preferred_element_type=jnp.float32)
        for half, col in enumerate((r, depth + r)):
            here = slice(half * rows, (half + 1) * rows)
            out_s[pl.ds(col, rows, stride=cols), :] = gate[pl.ds(col * rows, rows)] * o[here]
    parts = sems.shape[0]
    step = rows // parts
    copies = []
    for p in range(parts):
        here = pl.ds(p * step * cols, step * cols)
        out_v[pl.ds(p * step, step)] = (
            out_s[here].astype(jnp.bfloat16).reshape(step, cols, width)
        )
        copies.append(
            pltpu.make_async_copy(
                out_v.at[pl.ds(p * step, step)], out_hbm.at[pl.ds(p * step, step)], sems.at[p]
            )
        )
        copies[-1].start()
    for copy in copies:
        copy.wait()


SMEM = pl.BlockSpec(memory_space=pltpu.SMEM)
VMEM = pl.BlockSpec(memory_space=pltpu.VMEM)
HBM = pl.BlockSpec(memory_space=pltpu.HBM)
COST = pl.CostEstimate(flops=2**30, bytes_accessed=2**20, transcendentals=0)
PARAMS = pltpu.CompilerParams(vmem_limit_bytes=16 * 2**20)


def body(pair, lengths, ln_gain, ln_bias, w_ab, w_gate, out_gain, out_bias, w_out):
    rows, cols, width = pair.shape
    hidden = w_out.shape[0]
    steps, blocks, cores = (lax.axis_size(a) for a in ("gy", "gx", "gz"))
    parts = 4
    flat, square = (rows * cols, width), (hidden, 2 * rows)
    centered = pl.pallas_call(
        center_kernel,
        out_shape=jax.ShapeDtypeStruct((cols, rows, width), jnp.float32),
        in_specs=[VMEM],
        out_specs=VMEM,
        scratch_shapes=[pltpu.VMEM(flat, jnp.float32)],
        compiler_params=PARAMS,
        cost_estimate=COST,
        name="center",
    )(pair)
    normed, operands = pl.pallas_call(
        pre_kernel,
        out_shape=(
            jax.ShapeDtypeStruct(flat, jnp.bfloat16),
            jax.ShapeDtypeStruct((hidden, cols, 2 * rows), jnp.bfloat16),
        ),
        in_specs=[VMEM] * 4,
        out_specs=(VMEM, VMEM),
        scratch_shapes=[pltpu.VMEM((hidden * cols, 2 * rows), jnp.float32)],
        compiler_params=PARAMS,
        cost_estimate=COST,
        name="pre",
    )(centered, ln_gain[None], ln_bias[None], w_ab)
    own = lax.all_to_all(operands, ("gy", "gx"), 0, 0, tiled=True)
    own, lengths = lax.optimization_barrier((own, lengths))
    peer = lax.ppermute(own, "gz", [(g, cores - 1 - g) for g in range(cores)])
    shape = (steps, blocks, cols, 2 * rows)
    own, peer = own.reshape(shape), peer.reshape(shape)
    group = (blocks, rows // cols, blocks // 2, cols, 2 * rows)
    tiles, left, gate, gain_t, bias_t = pl.pallas_call(
        own_kernel,
        out_shape=(
            jax.ShapeDtypeStruct(group, jnp.bfloat16),
            jax.ShapeDtypeStruct((steps * cols, blocks * rows), jnp.bfloat16),
            jax.ShapeDtypeStruct(flat, jnp.float32),
            jax.ShapeDtypeStruct(square, jnp.float32),
            jax.ShapeDtypeStruct(square, jnp.float32),
        ),
        in_specs=[SMEM] + [VMEM] * 5,
        out_specs=(VMEM,) * 5,
        compiler_params=PARAMS,
        cost_estimate=COST,
        name="own",
    )(lengths, own, normed, w_gate, out_gain[None], out_bias[None])
    tiles = pl.pallas_call(
        peer_kernel,
        out_shape=jax.ShapeDtypeStruct((blocks, cores, *group[1:]), jnp.bfloat16),
        in_specs=[SMEM] + [VMEM] * 3,
        out_specs=VMEM,
        compiler_params=PARAMS,
        cost_estimate=COST,
        name="peer",
    )(lengths, left, peer, tiles)
    tiles = tiles.reshape(steps * blocks, cols // 2, 2 * rows)
    back = lax.all_to_all(tiles, ("gy", "gx"), 0, 0, tiled=True)
    return pl.pallas_call(
        post_kernel,
        out_shape=jax.ShapeDtypeStruct((rows, cols, width), jnp.bfloat16),
        in_specs=[VMEM] * 5,
        out_specs=HBM,
        scratch_shapes=[
            pltpu.VMEM((hidden * cols // 2, 2 * rows), jnp.float32),
            pltpu.VMEM(flat, jnp.float32),
            pltpu.VMEM((rows, cols, width), jnp.bfloat16),
            pltpu.SemaphoreType.DMA((parts,)),
        ],
        compiler_params=PARAMS,
        name="post",
    )(back.reshape(hidden // 2, cols, 2 * rows), gate, gain_t, bias_t, w_out)


def solution(mesh):
    in_specs = (P(("grp", "gx", "gz"), "gy", None), P("grp"), P(), P(), P(), P(), P(), P(), P())
    out_specs = P(("grp", "gx", "gz"), "gy", None)
    return jax.shard_map(body, mesh=mesh, in_specs=in_specs, out_specs=out_specs, check_vma=False)
```

```python
import functools

import jax
import jax.numpy as jnp
from jax import lax
from jax.experimental import pallas as pl
from jax.experimental.pallas import tpu as pltpu
from jax.sharding import PartitionSpec as P

NT = (((1,), (1,)), ((), ()))
TN = (((0,), (0,)), ((), ()))
EPS = 1e-05


def low_half(shape):
    return lax.broadcasted_iota(jnp.int32, shape, len(shape) - 1) < shape[-1] // 2


def swap_halves(value):
    return pltpu.roll(value, value.shape[-1] // 2, value.ndim - 1)


def center_kernel(x_ref, out_ref, rows_s):
    cols, rows, width = out_ref.shape
    x = x_ref[...].reshape(rows * cols, width).astype(jnp.float32)
    x = x - jnp.mean(x, -1, keepdims=True)
    spread = jnp.mean(x * x, -1, keepdims=True)
    rows_s[...] = x * lax.rsqrt(spread + EPS)
    for k in range(cols):
        out_ref[k] = rows_s[pl.ds(k, rows, stride=cols), :]


def pre_kernel(x_ref, gain, bias, w_ref, normed_ref, out_ref, out_s):
    cols, rows, width = x_ref.shape
    hidden = out_ref.shape[0]
    w_t = w_ref[...].astype(jnp.float32).T.astype(jnp.bfloat16)
    low = low_half((1, 2 * rows))
    for k in range(0, cols, 2):
        block = x_ref[pl.ds(k, 2)].reshape(2 * rows, width)
        block = (block * gain[...] + bias[...]).astype(jnp.bfloat16)
        normed_ref[pl.ds(k * rows, 2 * rows)] = block
        proj = lax.dot_general(w_t, block, NT, preferred_element_type=jnp.float32)
        left = jax.nn.sigmoid(proj[:hidden]) * proj[hidden : 2 * hidden]
        right = jax.nn.sigmoid(proj[2 * hidden : 3 * hidden]) * proj[3 * hidden :]
        out_s[pl.ds(k, hidden, stride=cols), :] = jnp.where(low, left, swap_halves(right))
        out_s[pl.ds(k + 1, hidden, stride=cols), :] = jnp.where(low, swap_halves(left), right)
    out_ref[...] = out_s[...].astype(jnp.bfloat16).reshape(out_ref.shape)


def side():
    return lax.rem(lax.axis_index("gx") + lax.axis_index("gz"), lax.axis_size("gz"))


def core_of(group, block):
    return lax.rem(group + block, lax.axis_size("gz"))


def operand(ref, first, length, group, mask_k):
    steps, blocks, depth, lanes = ref.shape
    half = lanes // 2
    parts = [ref[:, x].reshape(steps * depth, lanes)[:, first : first + half] for x in range(blocks)]
    value = jnp.concatenate(parts, 1)
    lane = lax.broadcasted_iota(jnp.int32, (1, blocks * half), 1)
    block = lane // half
    live = (block * lax.axis_size("gz") + core_of(group, block)) * half + lane % half < length
    if mask_k:
        live = live & (lax.broadcasted_iota(jnp.int32, (steps * depth, 1), 0) < length)
    return value * jnp.where(live, 1.0, 0.0).astype(jnp.bfloat16)


def product(left, right, depth):
    lanes = 2 * left.shape[1] // 4
    half = lanes // 2
    low = low_half((1, 1, lanes))
    total = lax.dot_general(right, left, TN, preferred_element_type=jnp.float32)
    blocks = total.shape[1] // half
    total = total.reshape(total.shape[0] // depth, depth, blocks * half)
    top, bottom = total[:, : depth // 2], total[:, depth // 2 :]
    tiles = []
    for pair in range(blocks // 2):
        here = slice(pair * lanes, (pair + 1) * lanes)
        even = jnp.where(low, top[..., here], swap_halves(bottom[..., here]))
        odd = jnp.where(low, swap_halves(top[..., here]), bottom[..., here])
        tiles.append(jnp.concatenate([even, odd], 1).astype(jnp.bfloat16))
    return [t.reshape(blocks, t.shape[0] // blocks, depth, lanes) for t in tiles]


def own_kernel(length, own_ref, normed, w_gate, gain, bias, out_ref, left_ref, gate_ref, gain_t, bias_t):
    half = own_ref.shape[3] // 2
    group = side()
    left = operand(own_ref, 0, length[0], group, True)
    left_ref[...] = left
    tiles = product(left, operand(own_ref, half, length[0], group, False), own_ref.shape[2])
    for pair, tile in enumerate(tiles):
        out_ref[:, :, pair] = tile
    gate_ref[...] = jax.nn.sigmoid(jnp.dot(normed[...], w_gate[...], preferred_element_type=jnp.float32))
    gain_t[...] = jnp.broadcast_to(gain[...], gain_t.shape[::-1]).T
    bias_t[...] = jnp.broadcast_to(bias[...], bias_t.shape[::-1]).T


def peer_kernel(length, left_ref, peer_ref, done_ref, out_ref):
    half = peer_ref.shape[3] // 2
    group = side()
    right = operand(peer_ref, half, length[0], group + 1, False)
    tiles = product(left_ref[...], right, peer_ref.shape[2])
    for block in range(done_ref.shape[0]):
        out_ref[block, core_of(group, block)] = done_ref[block]
        for pair, tile in enumerate(tiles):
            out_ref[block, core_of(group, block + 1), :, pair] = tile[block]


def post_kernel(t_ref, gate, gain_t, bias_t, w_ref, out_hbm, t_s, out_s, out_v, sems):
    rows, cols, width = out_v.shape
    hidden = w_ref.shape[0]
    depth = cols // 2
    t_s[...] = t_ref[...].astype(jnp.float32).reshape(t_s.shape)
    w = w_ref[...]
    for r in range(depth):
        t = t_s[pl.ds(r, hidden, stride=depth), :]
        t = t - jnp.mean(t, 0, keepdims=True)
        spread = jnp.mean(t * t, 0, keepdims=True)
        t = (t * lax.rsqrt(spread + EPS) * gain_t[...] + bias_t[...]).astype(jnp.bfloat16)
        o = lax.dot_general(t, w, TN, preferred_element_type=jnp.float32)
        for half, col in enumerate((r, depth + r)):
            here = slice(half * rows, (half + 1) * rows)
            out_s[pl.ds(col, rows, stride=cols), :] = gate[pl.ds(col * rows, rows)] * o[here]
    parts = sems.shape[0]
    step = rows // parts
    copies = []
    for p in range(parts):
        here = pl.ds(p * step * cols, step * cols)
        out_v[pl.ds(p * step, step)] = (
            out_s[here].astype(jnp.bfloat16).reshape(step, cols, width)
        )
        copies.append(
            pltpu.make_async_copy(
                out_v.at[pl.ds(p * step, step)], out_hbm.at[pl.ds(p * step, step)], sems.at[p]
            )
        )
        copies[-1].start()
    for copy in copies:
        copy.wait()


SMEM = pl.BlockSpec(memory_space=pltpu.SMEM)
VMEM = pl.BlockSpec(memory_space=pltpu.VMEM)
HBM = pl.BlockSpec(memory_space=pltpu.HBM)
COST = pl.CostEstimate(flops=2**30, bytes_accessed=2**20, transcendentals=0)
PARAMS = pltpu.CompilerParams(vmem_limit_bytes=16 * 2**20)


def body(pair, lengths, ln_gain, ln_bias, w_ab, w_gate, out_gain, out_bias, w_out):
    rows, cols, width = pair.shape
    hidden = w_out.shape[0]
    steps, blocks, cores = (lax.axis_size(a) for a in ("gy", "gx", "gz"))
    parts = 4
    flat, square = (rows * cols, width), (hidden, 2 * rows)
    centered = pl.pallas_call(
        center_kernel,
        out_shape=jax.ShapeDtypeStruct((cols, rows, width), jnp.float32),
        in_specs=[VMEM],
        out_specs=VMEM,
        scratch_shapes=[pltpu.VMEM(flat, jnp.float32)],
        compiler_params=PARAMS,
        cost_estimate=COST,
        name="center",
    )(pair)
    normed, operands = pl.pallas_call(
        pre_kernel,
        out_shape=(
            jax.ShapeDtypeStruct(flat, jnp.bfloat16),
            jax.ShapeDtypeStruct((hidden, cols, 2 * rows), jnp.bfloat16),
        ),
        in_specs=[VMEM] * 4,
        out_specs=(VMEM, VMEM),
        scratch_shapes=[pltpu.VMEM((hidden * cols, 2 * rows), jnp.float32)],
        compiler_params=PARAMS,
        cost_estimate=COST,
        name="pre",
    )(centered, ln_gain[None], ln_bias[None], w_ab)
    groups = [
        [(z * blocks + x) * cores + (g + x) % cores for z in range(steps) for x in range(blocks)]
        for g in range(cores)
    ]

    def exchange(value):
        axes = ("gy", "gx", "gz")
        return lax.all_to_all(value, axes, 0, 0, tiled=True, axis_index_groups=groups)

    own = exchange(operands)
    own, lengths = lax.optimization_barrier((own, lengths))
    peer = lax.ppermute(own, "gz", [(g, cores - 1 - g) for g in range(cores)])
    shape = (steps, blocks, cols, 2 * rows)
    own, peer = own.reshape(shape), peer.reshape(shape)
    group = (blocks, rows // cols, blocks // 2, cols, 2 * rows)
    tiles, left, gate, gain_t, bias_t = pl.pallas_call(
        own_kernel,
        out_shape=(
            jax.ShapeDtypeStruct(group, jnp.bfloat16),
            jax.ShapeDtypeStruct((steps * cols, blocks * rows), jnp.bfloat16),
            jax.ShapeDtypeStruct(flat, jnp.float32),
            jax.ShapeDtypeStruct(square, jnp.float32),
            jax.ShapeDtypeStruct(square, jnp.float32),
        ),
        in_specs=[SMEM] + [VMEM] * 5,
        out_specs=(VMEM,) * 5,
        compiler_params=PARAMS,
        cost_estimate=COST,
        name="own",
    )(lengths, own, normed, w_gate, out_gain[None], out_bias[None])
    tiles = pl.pallas_call(
        peer_kernel,
        out_shape=jax.ShapeDtypeStruct((blocks, cores, *group[1:]), jnp.bfloat16),
        in_specs=[SMEM] + [VMEM] * 3,
        out_specs=VMEM,
        compiler_params=PARAMS,
        cost_estimate=COST,
        name="peer",
    )(lengths, left, peer, tiles)
    tiles = tiles.reshape(steps * blocks, cols // 2, 2 * rows)
    back = exchange(tiles)
    return pl.pallas_call(
        post_kernel,
        out_shape=jax.ShapeDtypeStruct((rows, cols, width), jnp.bfloat16),
        in_specs=[VMEM] * 5,
        out_specs=HBM,
        scratch_shapes=[
            pltpu.VMEM((hidden * cols // 2, 2 * rows), jnp.float32),
            pltpu.VMEM(flat, jnp.float32),
            pltpu.VMEM((rows, cols, width), jnp.bfloat16),
            pltpu.SemaphoreType.DMA((parts,)),
        ],
        compiler_params=PARAMS,
        name="post",
    )(back.reshape(hidden // 2, cols, 2 * rows), gate, gain_t, bias_t, w_out)


def solution(mesh):
    in_specs = (P(("grp", "gx", "gz"), "gy", None), P("grp"), P(), P(), P(), P(), P(), P(), P())
    out_specs = P(("grp", "gx", "gz"), "gy", None)
    return jax.shard_map(body, mesh=mesh, in_specs=in_specs, out_specs=out_specs, check_vma=False)
```

```python
import functools

import jax
import jax.numpy as jnp
from jax import lax
from jax.experimental import pallas as pl
from jax.experimental.pallas import tpu as pltpu
from jax.sharding import PartitionSpec as P

NT = (((1,), (1,)), ((), ()))
TN = (((0,), (0,)), ((), ()))
EPS = 1e-05


def low_half(shape):
    return lax.broadcasted_iota(jnp.int32, shape, len(shape) - 1) < shape[-1] // 2


def swap_halves(value):
    return pltpu.roll(value, value.shape[-1] // 2, value.ndim - 1)


def evens_first(rows, group):
    return [start + odd for start in range(0, rows, group) for odd in (0, 1)]


def center_kernel(x_ref, out_ref, rows_s):
    cols, rows, width = out_ref.shape
    x = x_ref[...].reshape(rows * cols, width).astype(jnp.float32)
    x = x - jnp.mean(x, -1, keepdims=True)
    spread = jnp.mean(x * x, -1, keepdims=True)
    rows_s[...] = x * lax.rsqrt(spread + EPS)
    for k in range(cols):
        for first, row in enumerate(evens_first(rows, cols)):
            out_ref[k, pl.ds(8 * first, 8)] = rows_s[pl.ds(row * cols + k, 8, stride=2 * cols), :]


def pre_kernel(x_ref, gain, bias, w_ref, normed_ref, out_ref, out_s):
    cols, rows, width = x_ref.shape
    hidden = out_ref.shape[0]
    w_t = w_ref[...].astype(jnp.float32).T.astype(jnp.bfloat16)
    low = low_half((1, 2 * rows))
    for k in range(0, cols, 2):
        block = x_ref[pl.ds(k, 2)].reshape(2 * rows, width)
        block = (block * gain[...] + bias[...]).astype(jnp.bfloat16)
        normed_ref[pl.ds(k * rows, 2 * rows)] = block
        proj = lax.dot_general(w_t, block, NT, preferred_element_type=jnp.float32)
        left = jax.nn.sigmoid(proj[:hidden]) * proj[hidden : 2 * hidden]
        right = jax.nn.sigmoid(proj[2 * hidden : 3 * hidden]) * proj[3 * hidden :]
        out_s[pl.ds(k, hidden, stride=cols), :] = jnp.where(low, left, swap_halves(right))
        out_s[pl.ds(k + 1, hidden, stride=cols), :] = jnp.where(low, swap_halves(left), right)
    out_ref[...] = out_s[...].astype(jnp.bfloat16).reshape(out_ref.shape)


def operand(ref, first, length, core, mask_k):
    steps, blocks, depth, lanes = ref.shape
    half = lanes // 2
    parts = [ref[:, x].reshape(steps * depth, lanes)[:, first : first + half] for x in range(blocks)]
    value = jnp.concatenate(parts, 1)
    lane = lax.broadcasted_iota(jnp.int32, (1, blocks * half), 1)
    slot = lane % depth
    row = lane % half - slot + slot % (depth // 2) * 2 + slot // (depth // 2)
    live = lane // half * (lax.axis_size("gz") * half) + core * half + row < length
    if mask_k:
        live = live & (lax.broadcasted_iota(jnp.int32, (steps * depth, 1), 0) < length)
    return value * jnp.where(live, 1.0, 0.0).astype(jnp.bfloat16)


def product(left, right, depth):
    lanes = 2 * left.shape[1] // 4
    half = lanes // 2
    low = low_half((1, 1, lanes))
    total = lax.dot_general(right, left, TN, preferred_element_type=jnp.float32)
    blocks = total.shape[1] // half
    total = total.reshape(total.shape[0] // depth, depth, blocks * half)
    top, bottom = total[:, : depth // 2], total[:, depth // 2 :]
    tiles = []
    for pair in range(blocks // 2):
        here = slice(pair * lanes, (pair + 1) * lanes)
        even = jnp.where(low, top[..., here], swap_halves(bottom[..., here]))
        odd = jnp.where(low, swap_halves(top[..., here]), bottom[..., here])
        tiles.append(jnp.concatenate([even, odd], 1).astype(jnp.bfloat16))
    return [t.reshape(blocks, t.shape[0] // blocks, depth, lanes) for t in tiles]


def own_kernel(length, own_ref, normed, w_gate, gain, bias, out_ref, left_ref, gate_ref, gain_t, bias_t):
    half = own_ref.shape[3] // 2
    core = lax.axis_index("gz")
    left = operand(own_ref, 0, length[0], core, True)
    left_ref[...] = left
    tiles = product(left, operand(own_ref, half, length[0], core, False), own_ref.shape[2])
    for pair, tile in enumerate(tiles):
        out_ref[:, :, pair] = tile
    gate_ref[...] = jax.nn.sigmoid(jnp.dot(normed[...], w_gate[...], preferred_element_type=jnp.float32))
    gain_t[...] = jnp.broadcast_to(gain[...], gain_t.shape[::-1]).T
    bias_t[...] = jnp.broadcast_to(bias[...], bias_t.shape[::-1]).T


def peer_kernel(length, left_ref, peer_ref, done_ref, out_ref):
    half = peer_ref.shape[3] // 2
    core = lax.axis_index("gz")
    out_ref[:, core] = done_ref[...]
    right = operand(peer_ref, half, length[0], 1 - core, False)
    for pair, tile in enumerate(product(left_ref[...], right, peer_ref.shape[2])):
        out_ref[:, 1 - core, :, pair] = tile


def post_kernel(t_ref, gate, gain_t, bias_t, w_ref, out_hbm, t_s, out_s, out_v, sems):
    parts, rows, part, width = out_v.shape
    hidden = w_ref.shape[0]
    cols = parts * part
    depth = cols // 2
    t_s[...] = t_ref[...].astype(jnp.float32).reshape(t_s.shape)
    w = w_ref[...]
    copies = []
    for r in range(depth):
        t = t_s[pl.ds(r, hidden, stride=depth), :]
        t = t - jnp.mean(t, 0, keepdims=True)
        spread = jnp.mean(t * t, 0, keepdims=True)
        t = (t * lax.rsqrt(spread + EPS) * gain_t[...] + bias_t[...]).astype(jnp.bfloat16)
        o = lax.dot_general(t, w, TN, preferred_element_type=jnp.float32)
        for half in (0, 1):
            col = 2 * r + half
            value = gate[pl.ds(col * rows, rows)] * o[half * rows : (half + 1) * rows]
            p, here = divmod(col, part)
            for first, row in enumerate(evens_first(rows, cols)):
                out_s[p, pl.ds(row * part + here, 8, stride=2 * part), :] = value[8 * first : 8 * first + 8]
        if (2 * r + 2) % part == 0:
            out_v[p] = out_s[p].astype(jnp.bfloat16).reshape(rows, part, width)
            copies.append(
                pltpu.make_async_copy(out_v.at[p], out_hbm.at[:, pl.ds(p * part, part)], sems.at[p])
            )
            copies[-1].start()
    for copy in copies:
        copy.wait()


SMEM = pl.BlockSpec(memory_space=pltpu.SMEM)
VMEM = pl.BlockSpec(memory_space=pltpu.VMEM)
HBM = pl.BlockSpec(memory_space=pltpu.HBM)
COST = pl.CostEstimate(flops=2**30, bytes_accessed=2**20, transcendentals=0)
PARAMS = pltpu.CompilerParams(vmem_limit_bytes=16 * 2**20)


def body(pair, lengths, ln_gain, ln_bias, w_ab, w_gate, out_gain, out_bias, w_out):
    rows, cols, width = pair.shape
    hidden = w_out.shape[0]
    steps, blocks, cores = (lax.axis_size(a) for a in ("gy", "gx", "gz"))
    parts = 2
    flat, square = (rows * cols, width), (hidden, 2 * rows)
    centered = pl.pallas_call(
        center_kernel,
        out_shape=jax.ShapeDtypeStruct((cols, rows, width), jnp.float32),
        in_specs=[VMEM],
        out_specs=VMEM,
        scratch_shapes=[pltpu.VMEM(flat, jnp.float32)],
        compiler_params=PARAMS,
        cost_estimate=COST,
        name="center",
    )(pair)
    normed, operands = pl.pallas_call(
        pre_kernel,
        out_shape=(
            jax.ShapeDtypeStruct(flat, jnp.bfloat16),
            jax.ShapeDtypeStruct((hidden, cols, 2 * rows), jnp.bfloat16),
        ),
        in_specs=[VMEM] * 4,
        out_specs=(VMEM, VMEM),
        scratch_shapes=[pltpu.VMEM((hidden * cols, 2 * rows), jnp.float32)],
        compiler_params=PARAMS,
        cost_estimate=COST,
        name="pre",
    )(centered, ln_gain[None], ln_bias[None], w_ab)
    own = lax.all_to_all(operands, ("gy", "gx"), 0, 0, tiled=True)
    own, lengths = lax.optimization_barrier((own, lengths))
    peer = lax.ppermute(own, "gz", [(g, cores - 1 - g) for g in range(cores)])
    shape = (steps, blocks, cols, 2 * rows)
    own, peer = own.reshape(shape), peer.reshape(shape)
    group = (blocks, rows // cols, blocks // 2, cols, 2 * rows)
    tiles, left, gate, gain_t, bias_t = pl.pallas_call(
        own_kernel,
        out_shape=(
            jax.ShapeDtypeStruct(group, jnp.bfloat16),
            jax.ShapeDtypeStruct((steps * cols, blocks * rows), jnp.bfloat16),
            jax.ShapeDtypeStruct(flat, jnp.float32),
            jax.ShapeDtypeStruct(square, jnp.float32),
            jax.ShapeDtypeStruct(square, jnp.float32),
        ),
        in_specs=[SMEM] + [VMEM] * 5,
        out_specs=(VMEM,) * 5,
        compiler_params=PARAMS,
        cost_estimate=COST,
        name="own",
    )(lengths, own, normed, w_gate, out_gain[None], out_bias[None])
    tiles = pl.pallas_call(
        peer_kernel,
        out_shape=jax.ShapeDtypeStruct((blocks, cores, *group[1:]), jnp.bfloat16),
        in_specs=[SMEM] + [VMEM] * 3,
        out_specs=VMEM,
        compiler_params=PARAMS,
        cost_estimate=COST,
        name="peer",
    )(lengths, left, peer, tiles)
    tiles = tiles.reshape(steps * blocks, cols // 2, 2 * rows)
    back = lax.all_to_all(tiles, ("gy", "gx"), 0, 0, tiled=True)
    return pl.pallas_call(
        post_kernel,
        out_shape=jax.ShapeDtypeStruct((rows, cols, width), jnp.bfloat16),
        in_specs=[VMEM] * 5,
        out_specs=HBM,
        scratch_shapes=[
            pltpu.VMEM((hidden * cols // 2, 2 * rows), jnp.float32),
            pltpu.VMEM((parts, rows * cols // parts, width), jnp.float32),
            pltpu.VMEM((parts, rows, cols // parts, width), jnp.bfloat16),
            pltpu.SemaphoreType.DMA((parts,)),
        ],
        compiler_params=PARAMS,
        name="post",
    )(back.reshape(hidden // 2, cols, 2 * rows), gate, gain_t, bias_t, w_out)


def solution(mesh):
    in_specs = (P(("grp", "gx", "gz"), "gy", None), P("grp"), P(), P(), P(), P(), P(), P(), P())
    out_specs = P(("grp", "gx", "gz"), "gy", None)
    return jax.shard_map(body, mesh=mesh, in_specs=in_specs, out_specs=out_specs, check_vma=False)
```

```python
import functools

import jax
import jax.numpy as jnp
from jax import lax
from jax.experimental import pallas as pl
from jax.experimental.pallas import tpu as pltpu
from jax.sharding import PartitionSpec as P

NT = (((1,), (1,)), ((), ()))
TN = (((0,), (0,)), ((), ()))
EPS = 1e-05


def low_half(shape):
    return lax.broadcasted_iota(jnp.int32, shape, len(shape) - 1) < shape[-1] // 2


def swap_halves(value):
    return pltpu.roll(value, value.shape[-1] // 2, value.ndim - 1)


def evens_first(rows, group):
    return [start + odd for start in range(0, rows, group) for odd in (0, 1)]


def center_kernel(x_ref, out_ref):
    x = x_ref[...].reshape(out_ref.shape).astype(jnp.float32)
    x = x - jnp.mean(x, -1, keepdims=True)
    spread = jnp.mean(x * x, -1, keepdims=True)
    out_ref[...] = x * lax.rsqrt(spread + EPS)


def pre_kernel(x_ref, gain, bias, w_ref, normed_ref, out_ref, out_s):
    hidden, cols, rows = out_ref.shape
    rows = rows // 2
    w_t = w_ref[...].astype(jnp.float32).T.astype(jnp.bfloat16)
    low = low_half((1, 2 * rows))
    for k in range(0, cols, 2):
        starts = [row * cols + col for col in (k, k + 1) for row in evens_first(rows, cols)]
        block = jnp.concatenate([x_ref[pl.ds(start, 8, stride=2 * cols), :] for start in starts], 0)
        block = (block * gain[...] + bias[...]).astype(jnp.bfloat16)
        normed_ref[pl.ds(k * rows, 2 * rows)] = block
        proj = lax.dot_general(w_t, block, NT, preferred_element_type=jnp.float32)
        left = jax.nn.sigmoid(proj[:hidden]) * proj[hidden : 2 * hidden]
        right = jax.nn.sigmoid(proj[2 * hidden : 3 * hidden]) * proj[3 * hidden :]
        out_s[pl.ds(k, hidden, stride=cols), :] = jnp.where(low, left, swap_halves(right))
        out_s[pl.ds(k + 1, hidden, stride=cols), :] = jnp.where(low, swap_halves(left), right)
    out_ref[...] = out_s[...].astype(jnp.bfloat16).reshape(out_ref.shape)


def operand(ref, first, length, core, mask_k):
    steps, blocks, depth, lanes = ref.shape
    half = lanes // 2
    parts = [ref[:, x].reshape(steps * depth, lanes)[:, first : first + half] for x in range(blocks)]
    value = jnp.concatenate(parts, 1)
    lane = lax.broadcasted_iota(jnp.int32, (1, blocks * half), 1)
    slot = lane % depth
    row = lane % half - slot + slot % (depth // 2) * 2 + slot // (depth // 2)
    live = lane // half * (lax.axis_size("gz") * half) + core * half + row < length
    if mask_k:
        live = live & (lax.broadcasted_iota(jnp.int32, (steps * depth, 1), 0) < length)
    return value * jnp.where(live, 1.0, 0.0).astype(jnp.bfloat16)


def product(left, right, depth):
    lanes = 2 * left.shape[1] // 4
    half = lanes // 2
    low = low_half((1, 1, lanes))
    total = lax.dot_general(right, left, TN, preferred_element_type=jnp.float32)
    blocks = total.shape[1] // half
    total = total.reshape(total.shape[0] // depth, depth, blocks * half)
    top, bottom = total[:, : depth // 2], total[:, depth // 2 :]
    tiles = []
    for pair in range(blocks // 2):
        here = slice(pair * lanes, (pair + 1) * lanes)
        even = jnp.where(low, top[..., here], swap_halves(bottom[..., here]))
        odd = jnp.where(low, swap_halves(top[..., here]), bottom[..., here])
        tiles.append(jnp.concatenate([even, odd], 1).astype(jnp.bfloat16))
    return [t.reshape(blocks, t.shape[0] // blocks, depth, lanes) for t in tiles]


def own_kernel(length, own_ref, normed, w_gate, gain, bias, out_ref, left_ref, gate_ref, gain_t, bias_t):
    half = own_ref.shape[3] // 2
    core = lax.axis_index("gz")
    left = operand(own_ref, 0, length[0], core, True)
    left_ref[...] = left
    tiles = product(left, operand(own_ref, half, length[0], core, False), own_ref.shape[2])
    for pair, tile in enumerate(tiles):
        out_ref[:, :, pair] = tile
    gate_ref[...] = jax.nn.sigmoid(jnp.dot(normed[...], w_gate[...], preferred_element_type=jnp.float32))
    gain_t[...] = jnp.broadcast_to(gain[...], gain_t.shape[::-1]).T
    bias_t[...] = jnp.broadcast_to(bias[...], bias_t.shape[::-1]).T


def peer_kernel(length, left_ref, peer_ref, done_ref, out_ref):
    half = peer_ref.shape[3] // 2
    core = lax.axis_index("gz")
    out_ref[:, core] = done_ref[...]
    right = operand(peer_ref, half, length[0], 1 - core, False)
    for pair, tile in enumerate(product(left_ref[...], right, peer_ref.shape[2])):
        out_ref[:, 1 - core, :, pair] = tile


def post_kernel(t_ref, gate, gain_t, bias_t, w_ref, out_hbm, t_s, out_s, out_v, sems):
    parts, rows, part, width = out_v.shape
    hidden = w_ref.shape[0]
    cols = parts * part
    depth = cols // 2
    t_s[...] = t_ref[...].astype(jnp.float32).reshape(t_s.shape)
    w = w_ref[...]
    copies = []
    for r in range(depth):
        t = t_s[pl.ds(r, hidden, stride=depth), :]
        t = t - jnp.mean(t, 0, keepdims=True)
        spread = jnp.mean(t * t, 0, keepdims=True)
        t = (t * lax.rsqrt(spread + EPS) * gain_t[...] + bias_t[...]).astype(jnp.bfloat16)
        o = lax.dot_general(t, w, TN, preferred_element_type=jnp.float32)
        for half in (0, 1):
            col = 2 * r + half
            value = gate[pl.ds(col * rows, rows)] * o[half * rows : (half + 1) * rows]
            p, here = divmod(col, part)
            for first, row in enumerate(evens_first(rows, cols)):
                out_s[p, pl.ds(row * part + here, 8, stride=2 * part), :] = value[8 * first : 8 * first + 8]
        if (2 * r + 2) % part == 0:
            out_v[p] = out_s[p].astype(jnp.bfloat16).reshape(rows, part, width)
            copies.append(
                pltpu.make_async_copy(out_v.at[p], out_hbm.at[:, pl.ds(p * part, part)], sems.at[p])
            )
            copies[-1].start()
    for copy in copies:
        copy.wait()


SMEM = pl.BlockSpec(memory_space=pltpu.SMEM)
VMEM = pl.BlockSpec(memory_space=pltpu.VMEM)
HBM = pl.BlockSpec(memory_space=pltpu.HBM)
COST = pl.CostEstimate(flops=2**30, bytes_accessed=2**20, transcendentals=0)
PARAMS = pltpu.CompilerParams(vmem_limit_bytes=16 * 2**20)


def body(pair, lengths, ln_gain, ln_bias, w_ab, w_gate, out_gain, out_bias, w_out):
    rows, cols, width = pair.shape
    hidden = w_out.shape[0]
    steps, blocks, cores = (lax.axis_size(a) for a in ("gy", "gx", "gz"))
    parts = 2
    flat, square = (rows * cols, width), (hidden, 2 * rows)
    centered = pl.pallas_call(
        center_kernel,
        out_shape=jax.ShapeDtypeStruct(flat, jnp.float32),
        in_specs=[VMEM],
        out_specs=VMEM,
        compiler_params=PARAMS,
        cost_estimate=COST,
        name="center",
    )(pair)
    normed, operands = pl.pallas_call(
        pre_kernel,
        out_shape=(
            jax.ShapeDtypeStruct(flat, jnp.bfloat16),
            jax.ShapeDtypeStruct((hidden, cols, 2 * rows), jnp.bfloat16),
        ),
        in_specs=[VMEM] * 4,
        out_specs=(VMEM, VMEM),
        scratch_shapes=[pltpu.VMEM((hidden * cols, 2 * rows), jnp.float32)],
        compiler_params=PARAMS,
        cost_estimate=COST,
        name="pre",
    )(centered, ln_gain[None], ln_bias[None], w_ab)
    own = lax.all_to_all(operands, ("gy", "gx"), 0, 0, tiled=True)
    own, lengths = lax.optimization_barrier((own, lengths))
    peer = lax.ppermute(own, "gz", [(g, cores - 1 - g) for g in range(cores)])
    shape = (steps, blocks, cols, 2 * rows)
    own, peer = own.reshape(shape), peer.reshape(shape)
    group = (blocks, rows // cols, blocks // 2, cols, 2 * rows)
    tiles, left, gate, gain_t, bias_t = pl.pallas_call(
        own_kernel,
        out_shape=(
            jax.ShapeDtypeStruct(group, jnp.bfloat16),
            jax.ShapeDtypeStruct((steps * cols, blocks * rows), jnp.bfloat16),
            jax.ShapeDtypeStruct(flat, jnp.float32),
            jax.ShapeDtypeStruct(square, jnp.float32),
            jax.ShapeDtypeStruct(square, jnp.float32),
        ),
        in_specs=[SMEM] + [VMEM] * 5,
        out_specs=(VMEM,) * 5,
        compiler_params=PARAMS,
        cost_estimate=COST,
        name="own",
    )(lengths, own, normed, w_gate, out_gain[None], out_bias[None])
    tiles = pl.pallas_call(
        peer_kernel,
        out_shape=jax.ShapeDtypeStruct((blocks, cores, *group[1:]), jnp.bfloat16),
        in_specs=[SMEM] + [VMEM] * 3,
        out_specs=VMEM,
        compiler_params=PARAMS,
        cost_estimate=COST,
        name="peer",
    )(lengths, left, peer, tiles)
    tiles = tiles.reshape(steps * blocks, cols // 2, 2 * rows)
    back = lax.all_to_all(tiles, ("gy", "gx"), 0, 0, tiled=True)
    return pl.pallas_call(
        post_kernel,
        out_shape=jax.ShapeDtypeStruct((rows, cols, width), jnp.bfloat16),
        in_specs=[VMEM] * 5,
        out_specs=HBM,
        scratch_shapes=[
            pltpu.VMEM((hidden * cols // 2, 2 * rows), jnp.float32),
            pltpu.VMEM((parts, rows * cols // parts, width), jnp.float32),
            pltpu.VMEM((parts, rows, cols // parts, width), jnp.bfloat16),
            pltpu.SemaphoreType.DMA((parts,)),
        ],
        compiler_params=PARAMS,
        name="post",
    )(back.reshape(hidden // 2, cols, 2 * rows), gate, gain_t, bias_t, w_out)


def solution(mesh):
    in_specs = (P(("grp", "gx", "gz"), "gy", None), P("grp"), P(), P(), P(), P(), P(), P(), P())
    out_specs = P(("grp", "gx", "gz"), "gy", None)
    return jax.shard_map(body, mesh=mesh, in_specs=in_specs, out_specs=out_specs, check_vma=False)
```

```python
import functools

import jax
import jax.numpy as jnp
from jax import lax
from jax.experimental import pallas as pl
from jax.experimental.pallas import tpu as pltpu
from jax.sharding import PartitionSpec as P

NT = (((1,), (1,)), ((), ()))
TN = (((0,), (0,)), ((), ()))
EPS = 1e-05


def low_half(shape):
    return lax.broadcasted_iota(jnp.int32, shape, len(shape) - 1) < shape[-1] // 2


def swap_halves(value):
    return pltpu.roll(value, value.shape[-1] // 2, value.ndim - 1)


def sigmoid(value):
    return 0.5 * jnp.tanh(0.5 * value) + 0.5


def evens_first(rows, group):
    return [start + odd for start in range(0, rows, group) for odd in (0, 1)]


def center_kernel(x_ref, out_ref):
    x = x_ref[...].reshape(out_ref.shape).astype(jnp.float32)
    x = x - jnp.mean(x, -1, keepdims=True)
    spread = jnp.mean(x * x, -1, keepdims=True)
    out_ref[...] = x * lax.rsqrt(spread + EPS)


def pre_kernel(x_ref, gain, bias, w_ref, normed_ref, out_ref, out_s):
    hidden, cols, rows = out_ref.shape
    rows = rows // 2
    w_t = w_ref[...].astype(jnp.float32).T.astype(jnp.bfloat16)
    low = low_half((1, 2 * rows))
    for k in range(0, cols, 2):
        starts = [row * cols + col for col in (k, k + 1) for row in evens_first(rows, cols)]
        block = jnp.concatenate([x_ref[pl.ds(start, 8, stride=2 * cols), :] for start in starts], 0)
        block = (block * gain[...] + bias[...]).astype(jnp.bfloat16)
        normed_ref[pl.ds(k * rows, 2 * rows)] = block
        proj = lax.dot_general(w_t, block, NT, preferred_element_type=jnp.float32)
        left = sigmoid(proj[:hidden]) * proj[hidden : 2 * hidden]
        right = sigmoid(proj[2 * hidden : 3 * hidden]) * proj[3 * hidden :]
        out_s[pl.ds(k, hidden, stride=cols), :] = jnp.where(low, left, swap_halves(right))
        out_s[pl.ds(k + 1, hidden, stride=cols), :] = jnp.where(low, swap_halves(left), right)
    out_ref[...] = out_s[...].astype(jnp.bfloat16).reshape(out_ref.shape)


def operand(ref, first, length, core, mask_k):
    steps, blocks, depth, lanes = ref.shape
    half = lanes // 2
    parts = [ref[:, x].reshape(steps * depth, lanes)[:, first : first + half] for x in range(blocks)]
    value = jnp.concatenate(parts, 1)
    lane = lax.broadcasted_iota(jnp.int32, (1, blocks * half), 1)
    slot = lane % depth
    row = lane % half - slot + slot % (depth // 2) * 2 + slot // (depth // 2)
    live = lane // half * (lax.axis_size("gz") * half) + core * half + row < length
    if mask_k:
        live = live & (lax.broadcasted_iota(jnp.int32, (steps * depth, 1), 0) < length)
    return value * jnp.where(live, 1.0, 0.0).astype(jnp.bfloat16)


def product(left, right, depth):
    lanes = 2 * left.shape[1] // 4
    half = lanes // 2
    low = low_half((1, 1, lanes))
    total = lax.dot_general(right, left, TN, preferred_element_type=jnp.float32)
    blocks = total.shape[1] // half
    total = total.reshape(total.shape[0] // depth, depth, blocks * half)
    top, bottom = total[:, : depth // 2], total[:, depth // 2 :]
    tiles = []
    for pair in range(blocks // 2):
        here = slice(pair * lanes, (pair + 1) * lanes)
        even = jnp.where(low, top[..., here], swap_halves(bottom[..., here]))
        odd = jnp.where(low, swap_halves(top[..., here]), bottom[..., here])
        tiles.append(jnp.concatenate([even, odd], 1).astype(jnp.bfloat16))
    return [t.reshape(blocks, t.shape[0] // blocks, depth, lanes) for t in tiles]


def own_kernel(length, own_ref, normed, w_gate, gain, bias, out_ref, left_ref, gate_ref, gain_t, bias_t):
    half = own_ref.shape[3] // 2
    core = lax.axis_index("gz")
    left = operand(own_ref, 0, length[0], core, True)
    left_ref[...] = left
    tiles = product(left, operand(own_ref, half, length[0], core, False), own_ref.shape[2])
    for pair, tile in enumerate(tiles):
        out_ref[:, :, pair] = tile
    gate_ref[...] = sigmoid(jnp.dot(normed[...], w_gate[...], preferred_element_type=jnp.float32))
    gain_t[...] = jnp.broadcast_to(gain[...], gain_t.shape[::-1]).T
    bias_t[...] = jnp.broadcast_to(bias[...], bias_t.shape[::-1]).T


def peer_kernel(length, left_ref, peer_ref, done_ref, out_ref):
    half = peer_ref.shape[3] // 2
    core = lax.axis_index("gz")
    out_ref[:, core] = done_ref[...]
    right = operand(peer_ref, half, length[0], 1 - core, False)
    for pair, tile in enumerate(product(left_ref[...], right, peer_ref.shape[2])):
        out_ref[:, 1 - core, :, pair] = tile


def post_kernel(t_ref, gate, gain_t, bias_t, w_ref, out_hbm, t_s, out_s, out_v, sems):
    parts, rows, part, width = out_v.shape
    hidden = w_ref.shape[0]
    cols = parts * part
    depth = cols // 2
    t_s[...] = t_ref[...].astype(jnp.float32).reshape(t_s.shape)
    w = w_ref[...]
    copies = []
    for r in range(depth):
        t = t_s[pl.ds(r, hidden, stride=depth), :]
        t = t - jnp.mean(t, 0, keepdims=True)
        spread = jnp.mean(t * t, 0, keepdims=True)
        t = (t * lax.rsqrt(spread + EPS) * gain_t[...] + bias_t[...]).astype(jnp.bfloat16)
        o = lax.dot_general(t, w, TN, preferred_element_type=jnp.float32)
        for half in (0, 1):
            col = 2 * r + half
            value = gate[pl.ds(col * rows, rows)] * o[half * rows : (half + 1) * rows]
            p, here = divmod(col, part)
            for first, row in enumerate(evens_first(rows, cols)):
                out_s[p, pl.ds(row * part + here, 8, stride=2 * part), :] = value[8 * first : 8 * first + 8]
        if (2 * r + 2) % part == 0:
            out_v[p] = out_s[p].astype(jnp.bfloat16).reshape(rows, part, width)
            copies.append(
                pltpu.make_async_copy(out_v.at[p], out_hbm.at[:, pl.ds(p * part, part)], sems.at[p])
            )
            copies[-1].start()
    for copy in copies:
        copy.wait()


SMEM = pl.BlockSpec(memory_space=pltpu.SMEM)
VMEM = pl.BlockSpec(memory_space=pltpu.VMEM)
HBM = pl.BlockSpec(memory_space=pltpu.HBM)
COST = pl.CostEstimate(flops=2**30, bytes_accessed=2**20, transcendentals=0)
PARAMS = pltpu.CompilerParams(vmem_limit_bytes=16 * 2**20)


def body(pair, lengths, ln_gain, ln_bias, w_ab, w_gate, out_gain, out_bias, w_out):
    rows, cols, width = pair.shape
    hidden = w_out.shape[0]
    steps, blocks, cores = (lax.axis_size(a) for a in ("gy", "gx", "gz"))
    parts = 2
    flat, square = (rows * cols, width), (hidden, 2 * rows)
    centered = pl.pallas_call(
        center_kernel,
        out_shape=jax.ShapeDtypeStruct(flat, jnp.float32),
        in_specs=[VMEM],
        out_specs=VMEM,
        compiler_params=PARAMS,
        cost_estimate=COST,
        name="center",
    )(pair)
    normed, operands = pl.pallas_call(
        pre_kernel,
        out_shape=(
            jax.ShapeDtypeStruct(flat, jnp.bfloat16),
            jax.ShapeDtypeStruct((hidden, cols, 2 * rows), jnp.bfloat16),
        ),
        in_specs=[VMEM] * 4,
        out_specs=(VMEM, VMEM),
        scratch_shapes=[pltpu.VMEM((hidden * cols, 2 * rows), jnp.float32)],
        compiler_params=PARAMS,
        cost_estimate=COST,
        name="pre",
    )(centered, ln_gain[None], ln_bias[None], w_ab)
    own = lax.all_to_all(operands, ("gy", "gx"), 0, 0, tiled=True)
    own, lengths = lax.optimization_barrier((own, lengths))
    peer = lax.ppermute(own, "gz", [(g, cores - 1 - g) for g in range(cores)])
    shape = (steps, blocks, cols, 2 * rows)
    own, peer = own.reshape(shape), peer.reshape(shape)
    group = (blocks, rows // cols, blocks // 2, cols, 2 * rows)
    tiles, left, gate, gain_t, bias_t = pl.pallas_call(
        own_kernel,
        out_shape=(
            jax.ShapeDtypeStruct(group, jnp.bfloat16),
            jax.ShapeDtypeStruct((steps * cols, blocks * rows), jnp.bfloat16),
            jax.ShapeDtypeStruct(flat, jnp.float32),
            jax.ShapeDtypeStruct(square, jnp.float32),
            jax.ShapeDtypeStruct(square, jnp.float32),
        ),
        in_specs=[SMEM] + [VMEM] * 5,
        out_specs=(VMEM,) * 5,
        compiler_params=PARAMS,
        cost_estimate=COST,
        name="own",
    )(lengths, own, normed, w_gate, out_gain[None], out_bias[None])
    tiles = pl.pallas_call(
        peer_kernel,
        out_shape=jax.ShapeDtypeStruct((blocks, cores, *group[1:]), jnp.bfloat16),
        in_specs=[SMEM] + [VMEM] * 3,
        out_specs=VMEM,
        compiler_params=PARAMS,
        cost_estimate=COST,
        name="peer",
    )(lengths, left, peer, tiles)
    tiles = tiles.reshape(steps * blocks, cols // 2, 2 * rows)
    back = lax.all_to_all(tiles, ("gy", "gx"), 0, 0, tiled=True)
    return pl.pallas_call(
        post_kernel,
        out_shape=jax.ShapeDtypeStruct((rows, cols, width), jnp.bfloat16),
        in_specs=[VMEM] * 5,
        out_specs=HBM,
        scratch_shapes=[
            pltpu.VMEM((hidden * cols // 2, 2 * rows), jnp.float32),
            pltpu.VMEM((parts, rows * cols // parts, width), jnp.float32),
            pltpu.VMEM((parts, rows, cols // parts, width), jnp.bfloat16),
            pltpu.SemaphoreType.DMA((parts,)),
        ],
        compiler_params=PARAMS,
        name="post",
    )(back.reshape(hidden // 2, cols, 2 * rows), gate, gain_t, bias_t, w_out)


def solution(mesh):
    in_specs = (P(("grp", "gx", "gz"), "gy", None), P("grp"), P(), P(), P(), P(), P(), P(), P())
    out_specs = P(("grp", "gx", "gz"), "gy", None)
    return jax.shard_map(body, mesh=mesh, in_specs=in_specs, out_specs=out_specs, check_vma=False)
```
